128 devices in a mesh: groups: 4 (over x, y), freq: 16 (over z), mgrp: 2 (over core).
Axes of the slice: x: 2, y: 2, z: 16, core: 2. Of those that a mesh axis runs over, the one named last changes fastest.
The devices are a block of a 8x8x16 slice.
Arguments:
- seeds: int32 [128, 1024], P('groups', 'mgrp'), parts along dimension 0, may hold values from 0 to 1073741823
- noise_amp: float32 [1024, 512], P(('groups', 'freq')), parts along dimension 0, may hold values from 0.3 to 3
- singular_projection: bfloat16 [128, 256, 16, 512], P('groups', 'freq'), parts along dimension 0, may hold values from -0.25 to 0.25
- kl_vecs: bfloat16 [128, 1536, 4096], P(('groups', 'freq'), 'mgrp'), parts along dimension 0, may hold values from -0.09375 to 0.09375
- m_order: int32 [128], P('groups'), parts along dimension 0, may hold values from 0 to 31, each once
- mode_counts: int32 [128], P('groups'), parts along dimension 0, may hold values from 384 to 1536, as said below
Outputs:
- kl_coeffs: bfloat16 [128, 1536, 1024], P(('groups', 'freq'), None, 'mgrp'), parts along dimension 0
The draws below stay inside these ranges and needn't reach their ends.
There are 4 independent parts, one for each index of `groups`. The reference program is written for one: setup_inputs(seed, part) draws one part's arguments, and reference() takes and returns one part's arrays. A program takes and returns all parts, laid end to end along the dimension named above; each array names one. Nothing has to cross between parts.
Inputs may be any that keep to these rules, and one draw needn't show every extreme that they name: `m_order`: each m appears in exactly one slot. `mode_counts`: some m keeps all 1536 modes.
All inputs are finite; a program needn't handle non-finite values.
Results may differ from the reference program's by a relative error of at most 0.0058.
Values may be sent and summed in bfloat16 or wider, within the bound.
A program may use at most 192 MiB of HBM per device.

```python
import math
import jax
import jax.numpy as jnp
from jax import lax

NF = 256
SVD_MODES = 16
NB = 512
KL_MAX = 1536
REALS = 1024
SVD_LEN = 4096
MS = 32


def draw_mode_counts(key, part):
    counts = jax.random.randint(key, (MS,), KL_MAX // 4, KL_MAX + 1, dtype=jnp.int32)
    chosen = jax.random.randint(jax.random.fold_in(key, 7), (), 0, MS, dtype=jnp.int32)
    return jnp.where(jnp.arange(MS, dtype=jnp.int32) == chosen, KL_MAX, counts).astype(jnp.int32)


def set_ends(array, key, least, top_value):
    place = [jax.random.randint(jax.random.fold_in(key, axis), (), 0, length) for axis, length in enumerate(array.shape)]
    main_axis = array.shape.index(max(array.shape))
    beside = place[:main_axis] + [(place[main_axis] + 1) % array.shape[main_axis]] + place[main_axis + 1:]
    return array.at[tuple(place)].set(least).at[tuple(beside)].set(top_value)


def shard_levels(rng, shape, shards, least, top_value):
    def one(axis_at, shards_of):
        draws = jax.random.uniform(jax.random.fold_in(jax.random.fold_in(rng, 6), axis_at), (shards_of,), jnp.float32, least / len(shards), top_value / len(shards))
        return jnp.repeat(jnp.exp(draws), shape[axis_at] // shards_of).reshape((-1,) + (1,) * (len(shape) - axis_at - 1))

    level = one(*shards[0])
    for cut in shards[1:]:
        level = level * one(*cut)
    return level


def normal_values(key, dims, scale, reach, shards=(), held_as=jnp.bfloat16):
    loudness = shard_levels(key, dims, shards, -0.22, 0.18) if shards else 1.0
    result = jax.random.normal(key, dims, jnp.float32) * scale * loudness
    return jnp.minimum(jnp.maximum(result, -reach), reach).astype(held_as)


def setup_inputs(seed: int = 0, part: int = 0) -> dict:
    key_list = jax.random.split(jax.random.key(seed), 7)
    own_keys = jax.random.split(jax.random.fold_in(key_list[6], part), 7)
    seeds = set_ends(jax.random.randint(own_keys[0], (MS, REALS), 0, 1073741824), jax.random.fold_in(own_keys[0], 1), 0, 1073741823).astype(jnp.int32)
    noise_amp = jnp.clip(jnp.exp(math.log(3.0) - 2.3025851 * jax.random.uniform(own_keys[1], (NF, NB), jnp.float32) ** shard_levels(own_keys[1], (NF, NB), ((0, 16),), -0.2, 0.2)), 0.3, 3.0)
    singular_projection = normal_values(own_keys[2], (MS, NF, SVD_MODES, NB), NB ** -0.5, 0.25, ((1, 16),))
    kl_vecs = normal_values(own_keys[3], (MS, KL_MAX, SVD_LEN), SVD_LEN ** -0.5, 0.09375, ((0, 16), (1, 2)))
    m_order = jax.random.permutation(own_keys[4], MS).astype(jnp.int32)
    mode_counts = draw_mode_counts(jax.random.fold_in(jax.random.fold_in(key_list[6], part), 71), part)
    return {"seeds": seeds, "noise_amp": noise_amp, "singular_projection": singular_projection, "kl_vecs": kl_vecs, "m_order": m_order, "mode_counts": mode_counts}


golden = 1640531527


def scramble(hashed_seed):
    hashed_seed = hashed_seed ^ ((hashed_seed >> 16) & 65535)
    hashed_seed = hashed_seed * 2146121005
    hashed_seed = hashed_seed ^ ((hashed_seed >> 15) & 131071)
    hashed_seed = hashed_seed * 1863026059
    hashed_seed = hashed_seed ^ ((hashed_seed >> 16) & 65535)
    return ((hashed_seed & 65535).astype(jnp.float32) - 32767.5) / 18918.0


def reference(seeds, noise_amp, singular_projection, kl_vecs, m_order, mode_counts):
    channel_index = jnp.arange(NF * NB, dtype=jnp.int32).reshape(NF, NB)
    mode_row_block = jnp.arange(KL_MAX, dtype=jnp.int32)

    def project(m_number):
        noise_draw = scramble(seeds[m_number][None, None, :] + channel_index[:, :, None] * golden)
        visible = (noise_amp[:, :, None] * noise_draw).astype(jnp.bfloat16)
        stacked = jnp.einsum("fkb,fbr->fkr", singular_projection[m_number].astype(jnp.float32), visible.astype(jnp.float32), precision=lax.Precision.HIGHEST)
        return stacked.astype(jnp.bfloat16).reshape(NF * SVD_MODES, REALS)

    def one_slot(position_index):
        m_number = m_order[position_index]
        vectors = project(m_number)
        coeffs = jnp.dot(kl_vecs[position_index], vectors, preferred_element_type=jnp.float32)
        kept_rows = mode_row_block[:, None] < mode_counts[m_number]
        return jnp.where(kept_rows, coeffs, jnp.float32(0.0)).astype(jnp.bfloat16)

    return lax.map(one_slot, jnp.arange(MS, dtype=jnp.int32))
```

```python
import functools
import math

import jax
import jax.numpy as jnp
from jax import lax
from jax.experimental import pallas as pl
from jax.experimental.pallas import tpu as pltpu
from jax.sharding import PartitionSpec as P

GOLDEN = 1640531527
MIX_A = 2146121005
MIX_B = 1863026059
MESH = pl.DeviceIdType.MESH
LANES = 128
ROWS = 128
NT = (((1,), (1,)), ((), ()))


def wrap(value):
    return (value + 2**31) % 2**32 - 2**31


def draw(x):
    x = x ^ lax.shift_right_logical(x, 16)
    x = x * MIX_A
    x = x ^ lax.shift_right_logical(x, 15)
    x = x * MIX_B
    x = x ^ lax.shift_right_logical(x, 16)
    return ((x & 65535).astype(jnp.float32) - 32767.5).astype(jnp.bfloat16)


def weigh_kernel(picked, projection, amp, out):
    del picked
    out[0] = (projection[0].astype(jnp.float32) * amp[...]).astype(jnp.bfloat16)


def weigh(picked, projection, amp):
    count = picked.shape[0]
    block = (1,) + projection.shape[1:]
    return pl.pallas_call(
        weigh_kernel,
        out_shape=jax.ShapeDtypeStruct((count,) + projection.shape[1:], jnp.bfloat16),
        grid_spec=pltpu.PrefetchScalarGridSpec(
            num_scalar_prefetch=1,
            grid=(count,),
            in_specs=[
                pl.BlockSpec(block, lambda d, picked: (picked[d], 0, 0, 0)),
                pl.BlockSpec(amp.shape, lambda d, picked: (0, 0, 0)),
            ],
            out_specs=pl.BlockSpec(block, lambda d, picked: (d, 0, 0, 0)),
        ),
        name="weigh",
    )(picked, projection, amp)


def project_kernel(
    size, base_ref, weights_ref, kl_ref, out_ref,
    base, wide, weights, kl, svd, coef, own, other,
    base_sem, weights_send, weights_recv, kl_own, kl_send, kl_recv, out_own, out_send, out_recv,
):
    z = lax.axis_index("freq")
    c = lax.axis_index("mgrp")
    partner = {"mgrp": 1 - c}
    channels, modes, entries = weights.shape[1:]
    reals = base.shape[0]
    half = reals // 2
    deep = channels * modes
    kept = kl.shape[1]
    share = kept // 2
    per_trip = LANES // modes
    trips = channels // per_trip
    slab = kept // trips

    def distance(j):
        return (j % 2) * ((j + 1) // 2) + (1 - j % 2) * ((size - j // 2) % size)

    def source(j):
        return (z - distance(j) + size) % size

    barrier = pltpu.get_barrier_semaphore()
    pl.semaphore_signal(barrier, inc=1, device_id=partner, device_id_type=MESH)
    for d in range(1, size):
        pl.semaphore_signal(barrier, inc=1, device_id={"freq": (z + d) % size}, device_id_type=MESH)

    own_weights = pltpu.make_async_copy(weights_ref.at[0], weights.at[0], weights_recv.at[0])
    own_weights.start()
    own_base = pltpu.make_async_copy(base_ref.at[0], base.at[pl.ds(0, half)], base_sem.at[0])
    own_base.start()
    kl[size] = jnp.zeros(kl.shape[1:], kl.dtype)
    svd[...] = jnp.zeros(svd.shape, svd.dtype)
    coef[...] = jnp.zeros(coef.shape, coef.dtype)
    pl.semaphore_wait(barrier, size)

    far_base = pltpu.make_async_remote_copy(
        src_ref=base_ref.at[1], dst_ref=base.at[pl.ds(half, half)], send_sem=base_sem.at[1], recv_sem=base_sem.at[2],
        device_id=partner, device_id_type=MESH,
    )
    far_base.start()

    def send_weights(d):
        return pltpu.make_async_remote_copy(
            src_ref=weights_ref.at[d], dst_ref=weights.at[d], send_sem=weights_send.at[d], recv_sem=weights_recv.at[d],
            device_id={"freq": (z + d) % size}, device_id_type=MESH,
        )

    def local_panel(tile):
        return pltpu.make_async_copy(
            kl_ref.at[c, :, pl.ds(pl.multiple_of(tile * deep, deep), deep)],
            kl.at[tile, pl.ds(pl.multiple_of(c * share, share), share)],
            kl_own.at[tile],
        )

    def send_panel(tile):
        return pltpu.make_async_remote_copy(
            src_ref=kl_ref.at[1 - c, :, pl.ds(pl.multiple_of(tile * deep, deep), deep)],
            dst_ref=kl.at[tile, pl.ds(pl.multiple_of(c * share, share), share)],
            send_sem=kl_send.at[tile], recv_sem=kl_recv.at[tile],
            device_id=partner, device_id_type=MESH,
        )

    @pl.loop(1, size)
    def _(j):
        send_weights(distance(j)).start()

    @pl.loop(0, size)
    def _(j):
        local_panel(source(j)).start()
        send_panel(source(j)).start()

    own_base.wait()
    far_base.wait()
    for b in range(entries // LANES):
        wide[:, b * LANES:(b + 1) * LANES] = base[...] + wrap(b * LANES * GOLDEN)

    @pl.loop(0, size)
    def _(j):
        cur = j % 2
        prev = 1 - cur
        at = distance(j)

        @pl.when(j == 0)
        def _():
            own_weights.wait()

        @pl.when(j > 0)
        def _():
            send_weights(at).wait_recv()
            local_panel(source(j - 1)).wait()
            send_panel(source(j - 1)).wait_recv()

        first = jnp.minimum(j, 1)
        tile = (1 - first) * size + first * source(jnp.maximum(j - 1, 0))
        start = source(j) * channels

        @pl.loop(0, trips)
        def _(t):
            rows = []
            for u in range(per_trip):
                before = [jnp.zeros((u * modes, entries), jnp.bfloat16)] if u else []
                after = [jnp.zeros((LANES - (u + 1) * modes, entries), jnp.bfloat16)] if u + 1 < per_trip else []
                rows.append(jnp.concatenate(before + [weights[at, t * per_trip + u]] + after, 0))
            stacked = jnp.concatenate(rows, 1)
            top = pl.multiple_of(t * slab, slab)
            blocks = reals // ROWS
            wide_n = 2 * ROWS
            for r in range(blocks):
                here = slice(r * ROWS, (r + 1) * ROWS)
                if r % 2 == 0:
                    there = slice(r * ROWS, r * ROWS + wide_n)
                    coef[pl.ds(top, slab), there] += lax.dot_general(
                        kl[tile, pl.ds(top, slab), :], svd[prev, there, :], NT, preferred_element_type=jnp.float32
                    )
                visible = jnp.concatenate(
                    [
                        draw(wide[here, :] + (start + t * per_trip + u) * wrap(entries * GOLDEN))
                        for u in range(per_trip)
                    ],
                    1,
                )
                projected = lax.dot_general(visible, stacked, NT, preferred_element_type=jnp.float32)
                svd[cur, here, pl.ds(pl.multiple_of(t * LANES, LANES), LANES)] = projected.astype(jnp.bfloat16)

    local_panel(source(size - 1)).wait()
    send_panel(source(size - 1)).wait_recv()

    parts = out_own.shape[0]
    piece = kept // parts

    def keep(i):
        return pltpu.make_async_copy(
            own.at[pl.ds(i * piece, piece)], out_ref.at[c, pl.ds(i * piece, piece)], out_own.at[i]
        )

    def hand(i):
        return pltpu.make_async_remote_copy(
            src_ref=other.at[pl.ds(i * piece, piece)], dst_ref=out_ref.at[c, pl.ds(i * piece, piece)],
            send_sem=out_send.at[i], recv_sem=out_recv.at[i], device_id=partner, device_id_type=MESH,
        )

    last = source(size - 1)
    for i in range(parts):
        here = slice(i * piece, (i + 1) * piece)
        for side, target in ((0, own), (1, other)):
            there = slice(side * half, (side + 1) * half)
            target[here, :] = (
                coef[here, there]
                + lax.dot_general(
                    kl[last, here, :], svd[(size - 1) % 2, there, :], NT, preferred_element_type=jnp.float32
                )
            ).astype(jnp.bfloat16)
        if i:
            keep(i - 1).start()
            hand(i - 1).start()
    keep(parts - 1).start()
    hand(parts - 1).start()

    @pl.loop(1, size)
    def _(d):
        send_weights(d).wait_send()

    @pl.loop(0, size)
    def _(tile):
        send_panel(tile).wait_send()

    for i in range(parts):
        keep(i).wait()
        hand(i).wait()


def project(size, base, weights, kl_vecs, reals):
    slots, share, length = kl_vecs.shape
    kept = 2 * share
    channels, modes, entries = weights.shape[1:]
    deep = channels * modes
    half = reals // 2
    parts = 6
    dma = pltpu.SemaphoreType.DMA
    return pl.pallas_call(
        functools.partial(project_kernel, size),
        out_shape=jax.ShapeDtypeStruct((slots, kept, half), jnp.bfloat16),
        in_specs=[pl.BlockSpec(memory_space=pl.ANY)] * 3,
        out_specs=pl.BlockSpec(memory_space=pl.ANY),
        scratch_shapes=[
            pltpu.VMEM((reals, LANES), jnp.int32),
            pltpu.VMEM((reals, entries), jnp.int32),
            pltpu.VMEM((size, channels, modes, entries), jnp.bfloat16),
            pltpu.VMEM((size + 1, kept, deep), jnp.bfloat16),
            pltpu.VMEM((2, reals, deep), jnp.bfloat16),
            pltpu.VMEM((kept, reals), jnp.float32),
            pltpu.VMEM((kept, half), jnp.bfloat16),
            pltpu.VMEM((kept, half), jnp.bfloat16),
            dma((3,)),
            dma((size,)),
            dma((size,)),
            dma((size,)),
            dma((size,)),
            dma((size,)),
            dma((parts,)),
            dma((parts,)),
            dma((parts,)),
        ],
        compiler_params=pltpu.CompilerParams(
            collective_id=0, has_side_effects=True, vmem_limit_bytes=60 * 2**20
        ),
        name="project",
    )(base, weights, kl_vecs)


def per_device(seeds, noise_amp, singular_projection, kl_vecs, m_order, mode_counts):
    size = lax.axis_size("freq")
    z = lax.axis_index("freq")
    c = lax.axis_index("mgrp")
    slots, share, _ = kl_vecs.shape
    half = seeds.shape[1]

    ahead = (z + jnp.arange(size, dtype=jnp.int32)) % size
    picked = m_order[ahead * slots + c]
    amp = (noise_amp * (1.0 / 18918.0))[:, None, :]
    weights = weigh(picked, singular_projection, amp)

    mine = m_order[z * slots + (c + jnp.arange(slots, dtype=jnp.int32)) % slots]
    steps = jnp.arange(LANES, dtype=jnp.int32) * GOLDEN
    base = seeds[mine][:, :, None] + steps[None, None, :]

    coeffs = project(size, base, weights, kl_vecs, 2 * half)
    limits = mode_counts[m_order[z * slots + jnp.arange(slots, dtype=jnp.int32)]]
    row_index = jnp.arange(2 * share, dtype=jnp.int32)
    return jnp.where(row_index[None, :, None] < limits[:, None, None], coeffs, jnp.bfloat16(0))


def solution(mesh):
    placed = (
        P("groups", "mgrp"),
        P(("groups", "freq"), None),
        P("groups", "freq", None, None),
        P(("groups", "freq"), "mgrp", None),
        P("groups"),
        P("groups"),
    )
    return jax.shard_map(
        per_device,
        mesh=mesh,
        in_specs=placed,
        out_specs=P(("groups", "freq"), None, "mgrp"),
        check_vma=False,
    )
```

```python
import functools
import math

import jax
import jax.numpy as jnp
from jax import lax
from jax.experimental import pallas as pl
from jax.experimental.pallas import tpu as pltpu
from jax.sharding import PartitionSpec as P

GOLDEN = 1640531527
MIX_A = 2146121005
MIX_B = 1863026059
MESH = pl.DeviceIdType.MESH
LANES = 128
ROWS = 128
GATHERED = 4
CENTRE = 32767.5
NT = (((1,), (1,)), ((), ()))


def wrap(value):
    return (value + 2**31) % 2**32 - 2**31


def draw(x):
    x = x ^ lax.shift_right_logical(x, 16)
    x = x * MIX_A
    x = x ^ lax.shift_right_logical(x, 15)
    x = x * MIX_B
    x = x ^ lax.shift_right_logical(x, 16)
    return (x & 65535).astype(jnp.float32).astype(jnp.bfloat16)


def weigh_kernel(order, place, *refs):
    del order, place
    *projections, amp, out = refs
    for i, projection in enumerate(projections):
        for f in range(amp.shape[0]):
            level = amp[f:f + 1, :] * (1.0 / 18918.0)
            out[i, f] = (projection[0, f].astype(jnp.float32) * level).astype(jnp.bfloat16)


def weigh(order, place, size, slots, projection, amp):
    block = (1,) + projection.shape[1:]

    def pick(i):
        def index(d, order, place):
            chip = lax.rem(place[0] + d * GATHERED + i, size)
            return order[chip * slots + place[1]], 0, 0, 0

        return index

    return pl.pallas_call(
        weigh_kernel,
        out_shape=jax.ShapeDtypeStruct((size,) + projection.shape[1:], jnp.bfloat16),
        grid_spec=pltpu.PrefetchScalarGridSpec(
            num_scalar_prefetch=2,
            grid=(size // GATHERED,),
            in_specs=[pl.BlockSpec(block, pick(i)) for i in range(GATHERED)]
            + [pl.BlockSpec(amp.shape, lambda d, order, place: (0, 0))],
            out_specs=pl.BlockSpec((GATHERED,) + projection.shape[1:], lambda d, order, place: (d, 0, 0, 0)),
        ),
        name="weigh",
    )(order, place, *[projection] * GATHERED, amp)


def project_kernel(
    size, base_ref, weights_ref, kl_ref, out_ref,
    base, wide, weights, kl, svd, coef, own, other,
    base_sem, weights_send, weights_recv, kl_own, kl_send, kl_recv, out_own, out_send, out_recv,
):
    z = lax.axis_index("freq")
    c = lax.axis_index("mgrp")
    partner = {"mgrp": 1 - c}
    channels, modes, entries = weights.shape[1:]
    reals = base.shape[0]
    half = reals // 2
    deep = channels * modes
    kept = kl.shape[1]
    share = kept // 2
    per_trip = LANES // modes
    trips = channels // per_trip
    slab = kept // trips

    def distance(j):
        return (j % 2) * ((j + 1) // 2) + (1 - j % 2) * ((size - j // 2) % size)

    def source(j):
        return (z - distance(j) + size) % size

    barrier = pltpu.get_barrier_semaphore()
    pl.semaphore_signal(barrier, inc=1, device_id=partner, device_id_type=MESH)
    for d in range(1, size):
        pl.semaphore_signal(barrier, inc=1, device_id={"freq": (z + d) % size}, device_id_type=MESH)

    own_weights = pltpu.make_async_copy(weights_ref.at[0], weights.at[0], weights_recv.at[0])
    own_weights.start()
    own_base = pltpu.make_async_copy(base_ref.at[0], base.at[pl.ds(0, half)], base_sem.at[0])
    own_base.start()
    kl[size] = jnp.zeros(kl.shape[1:], kl.dtype)
    svd[...] = jnp.zeros(svd.shape, svd.dtype)
    coef[...] = jnp.zeros(coef.shape, coef.dtype)
    pl.semaphore_wait(barrier, size)

    far_base = pltpu.make_async_remote_copy(
        src_ref=base_ref.at[1], dst_ref=base.at[pl.ds(half, half)], send_sem=base_sem.at[1], recv_sem=base_sem.at[2],
        device_id=partner, device_id_type=MESH,
    )
    far_base.start()

    def send_weights(d):
        return pltpu.make_async_remote_copy(
            src_ref=weights_ref.at[d], dst_ref=weights.at[d], send_sem=weights_send.at[d], recv_sem=weights_recv.at[d],
            device_id={"freq": (z + d) % size}, device_id_type=MESH,
        )

    def local_panel(tile):
        return pltpu.make_async_copy(
            kl_ref.at[c, :, pl.ds(pl.multiple_of(tile * deep, deep), deep)],
            kl.at[tile, pl.ds(pl.multiple_of(c * share, share), share)],
            kl_own.at[tile],
        )

    def send_panel(tile):
        return pltpu.make_async_remote_copy(
            src_ref=kl_ref.at[1 - c, :, pl.ds(pl.multiple_of(tile * deep, deep), deep)],
            dst_ref=kl.at[tile, pl.ds(pl.multiple_of(c * share, share), share)],
            send_sem=kl_send.at[tile], recv_sem=kl_recv.at[tile],
            device_id=partner, device_id_type=MESH,
        )

    @pl.loop(1, size)
    def _(j):
        send_weights(distance(j)).start()

    @pl.loop(0, size)
    def _(j):
        local_panel(source(j)).start()
        send_panel(source(j)).start()

    own_base.wait()
    far_base.wait()
    for b in range(entries // LANES):
        wide[:, b * LANES:(b + 1) * LANES] = base[...] + wrap(b * LANES * GOLDEN)

    @pl.loop(0, size)
    def _(j):
        cur = j % 2
        prev = 1 - cur
        at = distance(j)

        @pl.when(j == 0)
        def _():
            own_weights.wait()

        @pl.when(j > 0)
        def _():
            send_weights(at).wait_recv()
            local_panel(source(j - 1)).wait()
            send_panel(source(j - 1)).wait_recv()

        first = jnp.minimum(j, 1)
        tile = (1 - first) * size + first * source(jnp.maximum(j - 1, 0))
        start = source(j) * channels

        @pl.loop(0, trips)
        def _(t):
            rows = []
            for u in range(per_trip):
                before = [jnp.zeros((u * modes, entries), jnp.bfloat16)] if u else []
                after = [jnp.zeros((LANES - (u + 1) * modes, entries), jnp.bfloat16)] if u + 1 < per_trip else []
                rows.append(jnp.concatenate(before + [weights[at, t * per_trip + u]] + after, 0))
            stacked = jnp.concatenate(rows, 1)
            ones = jnp.ones((16, per_trip * entries), jnp.bfloat16)
            total = lax.dot_general(ones, stacked, NT, preferred_element_type=jnp.float32)
            shift = total[0:1, :] * CENTRE
            top = pl.multiple_of(t * slab, slab)
            blocks = reals // ROWS
            wide_n = 2 * ROWS
            for r in range(blocks):
                here = slice(r * ROWS, (r + 1) * ROWS)
                if r % 2 == 0:
                    there = slice(r * ROWS, r * ROWS + wide_n)
                    coef[pl.ds(top, slab), there] += lax.dot_general(
                        kl[tile, pl.ds(top, slab), :], svd[prev, there, :], NT, preferred_element_type=jnp.float32
                    )
                visible = jnp.concatenate(
                    [
                        draw(wide[here, :] + (start + t * per_trip + u) * wrap(entries * GOLDEN))
                        for u in range(per_trip)
                    ],
                    1,
                )
                projected = lax.dot_general(visible, stacked, NT, preferred_element_type=jnp.float32) - shift
                svd[cur, here, pl.ds(pl.multiple_of(t * LANES, LANES), LANES)] = projected.astype(jnp.bfloat16)

    local_panel(source(size - 1)).wait()
    send_panel(source(size - 1)).wait_recv()

    parts = out_own.shape[0]
    piece = kept // parts

    def keep(i):
        return pltpu.make_async_copy(
            own.at[pl.ds(i * piece, piece)], out_ref.at[c, pl.ds(i * piece, piece)], out_own.at[i]
        )

    def hand(i):
        return pltpu.make_async_remote_copy(
            src_ref=other.at[pl.ds(i * piece, piece)], dst_ref=out_ref.at[c, pl.ds(i * piece, piece)],
            send_sem=out_send.at[i], recv_sem=out_recv.at[i], device_id=partner, device_id_type=MESH,
        )

    last = source(size - 1)
    for i in range(parts):
        here = slice(i * piece, (i + 1) * piece)
        for side, target in ((0, own), (1, other)):
            there = slice(side * half, (side + 1) * half)
            target[here, :] = (
                coef[here, there]
                + lax.dot_general(
                    kl[last, here, :], svd[(size - 1) % 2, there, :], NT, preferred_element_type=jnp.float32
                )
            ).astype(jnp.bfloat16)
        if i:
            keep(i - 1).start()
            hand(i - 1).start()
    keep(parts - 1).start()
    hand(parts - 1).start()

    @pl.loop(1, size)
    def _(d):
        send_weights(d).wait_send()

    @pl.loop(0, size)
    def _(tile):
        send_panel(tile).wait_send()

    for i in range(parts):
        keep(i).wait()
        hand(i).wait()


def project(size, base, weights, kl_vecs, reals):
    slots, share, length = kl_vecs.shape
    kept = 2 * share
    channels, modes, entries = weights.shape[1:]
    deep = channels * modes
    half = reals // 2
    parts = 6
    dma = pltpu.SemaphoreType.DMA
    return pl.pallas_call(
        functools.partial(project_kernel, size),
        out_shape=jax.ShapeDtypeStruct((slots, kept, half), jnp.bfloat16),
        in_specs=[pl.BlockSpec(memory_space=pl.ANY)] * 3,
        out_specs=pl.BlockSpec(memory_space=pl.ANY),
        scratch_shapes=[
            pltpu.VMEM((reals, LANES), jnp.int32),
            pltpu.VMEM((reals, entries), jnp.int32),
            pltpu.VMEM((size, channels, modes, entries), jnp.bfloat16),
            pltpu.VMEM((size + 1, kept, deep), jnp.bfloat16),
            pltpu.VMEM((2, reals, deep), jnp.bfloat16),
            pltpu.VMEM((kept, reals), jnp.float32),
            pltpu.VMEM((kept, half), jnp.bfloat16),
            pltpu.VMEM((kept, half), jnp.bfloat16),
            dma((3,)),
            dma((size,)),
            dma((size,)),
            dma((size,)),
            dma((size,)),
            dma((size,)),
            dma((parts,)),
            dma((parts,)),
            dma((parts,)),
        ],
        compiler_params=pltpu.CompilerParams(
            collective_id=0, has_side_effects=True, vmem_limit_bytes=60 * 2**20
        ),
        name="project",
    )(base, weights, kl_vecs)


def per_device(seeds, noise_amp, singular_projection, kl_vecs, m_order, mode_counts):
    size = lax.axis_size("freq")
    z = lax.axis_index("freq")
    c = lax.axis_index("mgrp")
    slots, share, _ = kl_vecs.shape
    half = seeds.shape[1]

    place = jnp.stack([z, c]).astype(jnp.int32)
    weights = weigh(m_order, place, size, slots, singular_projection, noise_amp)

    mine = m_order[z * slots + (c + jnp.arange(slots, dtype=jnp.int32)) % slots]
    steps = jnp.arange(LANES, dtype=jnp.int32) * GOLDEN
    base = seeds[mine][:, :, None] + steps[None, None, :]

    coeffs = project(size, base, weights, kl_vecs, 2 * half)
    limits = mode_counts[mine]
    limits = jnp.where(c == 0, limits, limits[::-1])
    row_index = jnp.arange(2 * share, dtype=jnp.int32)
    return jnp.where(row_index[None, :, None] < limits[:, None, None], coeffs, jnp.bfloat16(0))


def solution(mesh):
    placed = (
        P("groups", "mgrp"),
        P(("groups", "freq"), None),
        P("groups", "freq", None, None),
        P(("groups", "freq"), "mgrp", None),
        P("groups"),
        P("groups"),
    )
    return jax.shard_map(
        per_device,
        mesh=mesh,
        in_specs=placed,
        out_specs=P(("groups", "freq"), None, "mgrp"),
        check_vma=False,
    )
```
